32 devices in a mesh: seq: 8 (over z, x), row: 2 (over core), col: 2 (over y).
Axes of the slice: x: 2, y: 2, z: 4, core: 2. Of those that a mesh axis runs over, the one named last changes fastest.
Arguments:
- tokens: bfloat16 [4096, 6144], P('seq', ('row', 'col')), may hold values from -20 to 20
- ln_gain: bfloat16 [6144], P(('row', 'col')), may hold values from 0.099609375 to 1.8984375
- ln_bias: bfloat16 [6144], P(('row', 'col')), may hold values from -1.5 to 1.5
- w_qkv: bfloat16 [3, 6144, 4096], P(None, 'row', 'col'), may hold values from -3 to 3
- w_out: bfloat16 [4096, 6144], P('col', 'row'), may hold values from -0.5 to 0.5
Outputs:
- attended: bfloat16 [4096, 6144], P('seq', ('row', 'col'))
The draws below stay inside these ranges and needn't reach their ends.
All inputs are finite; a program needn't handle non-finite values.
Results may differ from the reference program's by a relative error of at most 0.014.
Values may be sent and summed in bfloat16 or wider, within the bound.
A program may use at most 192 MiB of HBM per device.

```python
import math
import jax
import jax.numpy as jnp
from jax import lax

D = 6144
H = 32
HD = 128
T_SIZE = 4096


def draw_tokens(key, part):
    subkeys = jax.random.split(key, 3)
    group_size = max(D // 48, 1)
    group_count = D // group_size
    scale_levels = jnp.exp(jax.random.uniform(subkeys[0], (T_SIZE, group_count), jnp.float32, jnp.log(0.2), jnp.log(3.0)))
    scale_levels = jnp.repeat(scale_levels, group_size, axis=1)
    offsets = 0.5 * jnp.clip(jax.random.normal(subkeys[1], (T_SIZE, 1), jnp.float32), -4.0, 4.0)
    noise = jnp.clip(jax.random.normal(subkeys[2], (T_SIZE, D), jnp.float32), -4.0, 4.0)
    values = offsets + scale_levels * noise
    return values.astype(jnp.bfloat16)


def draw_w_qkv(key, part):
    subkeys = jax.random.split(key, 1)
    base = jnp.clip(jax.random.normal(subkeys[0], (3, D, H * HD), jnp.float32), -4.0, 4.0)
    factors = jnp.array([1.4, 1.4, 1.0], jnp.float32)[:, None, None] / jnp.sqrt(jnp.float32(D))
    weights = base * factors
    return weights.astype(jnp.bfloat16)


def steps_of(own_key, dims, pieces, low, high):
    level, own = 1.0, jax.random.fold_in(own_key, 6)
    for axis_at, parts in pieces:
        draws = jnp.exp(jax.random.uniform(jax.random.fold_in(own, axis_at), (parts,), jnp.float32, low / len(pieces), high / len(pieces)))
        level = level * jnp.repeat(draws, dims[axis_at] // parts).reshape([-1 if axis == axis_at else 1 for axis in range(len(dims))])
    return level


def normal_values(rng, shape, deviation, bound, cuts=(), kind=jnp.bfloat16):
    level = steps_of(rng, shape, cuts, -0.22, 0.18) if cuts else 1.0
    drawn = jax.random.normal(rng, shape, jnp.float32) * deviation * level
    return jnp.minimum(jnp.maximum(drawn, -bound), bound).astype(kind)


def setup_inputs(seed: int = 0) -> dict:
    seeds = jax.random.split(jax.random.key(seed), 6)
    tokens = draw_tokens(jax.random.fold_in(seeds[5], 71), 0)
    ln_gain = jnp.clip(1.0 + 0.18 * jax.random.normal(seeds[1], (D,), jnp.float32), 0.099609375, 1.8984375).astype(jnp.bfloat16)
    ln_bias = normal_values(seeds[2], (D,), 0.3, 1.5, ((0, 4),))
    w_qkv = draw_w_qkv(jax.random.fold_in(seeds[5], 71), 0)
    w_out = normal_values(seeds[4], (H * HD, D), HD ** -0.5, 0.5, ((0, 2), (1, 2)))
    return dict(tokens=tokens, ln_gain=ln_gain, ln_bias=ln_bias, w_qkv=w_qkv, w_out=w_out)


EPS = 0.25

def reference(tokens, ln_gain, ln_bias, w_qkv, w_out):
    as_float = tokens.astype(jnp.float32)
    token_mean = lax.optimization_barrier(jnp.sum(as_float, axis=1, keepdims=True)) / D
    meansq = lax.optimization_barrier(jnp.sum(as_float * as_float, axis=1, keepdims=True)) / D
    normed = ((as_float - token_mean) * lax.rsqrt(meansq - token_mean * token_mean + EPS) * ln_gain.astype(jnp.float32) + ln_bias.astype(jnp.float32)).astype(jnp.bfloat16)
    query_all = jnp.dot(normed, w_qkv[0], preferred_element_type=jnp.float32).astype(jnp.bfloat16)
    key_all = jnp.dot(normed, w_qkv[1], preferred_element_type=jnp.float32).astype(jnp.bfloat16)
    value_all = jnp.dot(normed, w_qkv[2], preferred_element_type=jnp.float32).astype(jnp.bfloat16)
    score_scale = 1.0 / math.sqrt(HD)

    def one_head(head_index):
        first_col = (head_index * HD).astype(jnp.int32)
        query_head = lax.dynamic_slice_in_dim(query_all, first_col, HD, 1)
        key_head = lax.dynamic_slice_in_dim(key_all, first_col, HD, 1)
        value_head = lax.dynamic_slice_in_dim(value_all, first_col, HD, 1)
        scores = jnp.dot(query_head, key_head.T, preferred_element_type=jnp.float32) * score_scale
        weights = jnp.exp(scores - lax.optimization_barrier(jnp.max(scores, axis=1, keepdims=True)))
        rowsum = lax.optimization_barrier(jnp.sum(weights, axis=1, keepdims=True))
        blended = jnp.dot(weights.astype(jnp.bfloat16), value_head, preferred_element_type=jnp.float32) / rowsum
        return blended.astype(jnp.bfloat16)
    per_head = lax.map(one_head, jnp.arange(H, dtype=jnp.int32))
    context = jnp.transpose(per_head, (1, 0, 2)).reshape(query_all.shape[0], H * HD)
    attended = as_float + jnp.dot(context, w_out, preferred_element_type=jnp.float32)
    return attended.astype(jnp.bfloat16)
```

```python
import functools
import math

import jax
import jax.numpy as jnp
from jax import lax
from jax.experimental import pallas as pl
from jax.experimental.pallas import tpu as pltpu
from jax.sharding import PartitionSpec as P

HD = 128
EPS = 0.25
IN_CHUNKS = 2
VMEM_LIMIT = 60 * 1024 * 1024


def params():
    return pltpu.CompilerParams(vmem_limit_bytes=VMEM_LIMIT)


def project_kernel(head_major, has_acc, idx_ref, x_ref, w_ref, *rest):
    if has_acc:
        acc_ref, out_ref = rest
    else:
        (out_ref,) = rest
    total = jnp.dot(x_ref[...], w_ref[0], preferred_element_type=jnp.float32)
    if has_acc:
        total = total + acc_ref[0]
    if head_major:
        for h in range(out_ref.shape[0]):
            out_ref[h, 0] = total[:, h * HD : (h + 1) * HD].astype(out_ref.dtype)
    else:
        out_ref[0] = total.astype(out_ref.dtype)


def project(x, w, acc, acc_row, row_block, col_block, width, dtype, head_major):
    rows, depth = x.shape
    bn = min(512, width)
    nb = width // bn
    idx = jnp.stack([jnp.int32(row_block), jnp.int32(col_block)])
    in_specs = [
        pl.BlockSpec((rows, depth), lambda k, j, i: (0, 0)),
        pl.BlockSpec((1, depth, bn), lambda k, j, i: (k, i[0], i[1] * nb + j)),
    ]
    args = [x, w]
    if acc is not None:
        in_specs.append(
            pl.BlockSpec((1, rows, bn), lambda k, j, i: (k, acc_row, i[1] * nb + j))
        )
        args.append(acc)
    if head_major:
        out_shape = jax.ShapeDtypeStruct((width // HD, 3, rows, HD), dtype)
        out_spec = pl.BlockSpec((bn // HD, 1, rows, HD), lambda k, j, i: (j, k, 0, 0))
    else:
        out_shape = jax.ShapeDtypeStruct((3, rows, width), dtype)
        out_spec = pl.BlockSpec((1, rows, bn), lambda k, j, i: (k, 0, j))
    return pl.pallas_call(
        functools.partial(project_kernel, head_major, acc is not None),
        grid_spec=pltpu.PrefetchScalarGridSpec(
            num_scalar_prefetch=1, grid=(3, nb), in_specs=in_specs, out_specs=out_spec
        ),
        out_shape=out_shape,
        compiler_params=params(),
        cost_estimate=pl.CostEstimate(
            flops=2 * rows * depth * width * 3,
            bytes_accessed=3 * width * (depth * 2 + rows * 8),
            transcendentals=0,
        ),
    )(idx, *args)


def attend_kernel(parts, q_ref, *refs):
    k_refs, v_refs, o_ref = refs[:parts], refs[parts : 2 * parts], refs[2 * parts]
    bs, tq = q_ref.shape[0], q_ref.shape[3]
    scale = math.log2(math.e) / math.sqrt(HD)
    q = q_ref[:, 0, 0].reshape(bs * tq, HD)
    top = acc = None
    for k_ref, v_ref in zip(k_refs, v_refs):
        sources, tk = k_ref.shape[0], k_ref.shape[3]
        step = max(1, min(sources, 1024 // tk))
        for first in range(0, sources, step):
            keys = k_ref[first : first + step, 0, 0].reshape(step * tk, HD)
            values = v_ref[first : first + step, 0, 0].reshape(step * tk, HD)
            values = jnp.concatenate([values, jnp.ones_like(values)], axis=1)
            scores = lax.dot_general(
                q, keys, (((1,), (1,)), ((), ())), preferred_element_type=jnp.float32
            )
            block_top = jnp.max(scores, axis=1, keepdims=True) * scale
            new_top = block_top if top is None else jnp.maximum(top, block_top)
            weights = jnp.exp2(scores * scale - new_top).astype(jnp.bfloat16)
            part = jnp.dot(weights, values, preferred_element_type=jnp.float32)
            acc = part if top is None else acc * jnp.exp2(top - new_top) + part
            top = new_top
    context = acc[:, :HD] / acc[:, HD:]
    o_ref[:, 0] = context.astype(o_ref.dtype).reshape(bs, tq, HD)


def attend(q, q_at, kvs, k_at):
    blocks, heads, _, tq, _ = q.shape
    bs = max(1, min(blocks, 512 // tq))

    def kv_spec(kv, at):
        shape = (kv.shape[0], 1, 1, kv.shape[3], HD)
        return pl.BlockSpec(shape, lambda h, i: (0, h, at, 0, 0))

    key_count = sum(kv.shape[0] * kv.shape[3] for kv in kvs)
    pairs = heads * blocks * tq * key_count
    return pl.pallas_call(
        functools.partial(attend_kernel, len(kvs)),
        grid=(heads, blocks // bs),
        in_specs=[pl.BlockSpec((bs, 1, 1, tq, HD), lambda h, i: (i, h, q_at, 0, 0))]
        + [kv_spec(kv, k_at) for kv in kvs]
        + [kv_spec(kv, k_at + 1) for kv in kvs],
        out_specs=pl.BlockSpec((bs, 1, tq, HD), lambda h, i: (i, h, 0, 0)),
        out_shape=jax.ShapeDtypeStruct((blocks, heads, tq, HD), jnp.bfloat16),
        compiler_params=params(),
        cost_estimate=pl.CostEstimate(
            flops=8 * pairs * HD,
            bytes_accessed=4 * heads * key_count * HD + 4 * heads * blocks * tq * HD,
            transcendentals=pairs,
        ),
    )(q, *kvs, *kvs)


def output_kernel(idx_ref, mine_ref, other_ref, w_ref, out_ref):
    def rows_of(ref):
        return jnp.concatenate([ref[h] for h in range(ref.shape[0])], axis=1)

    depth = mine_ref.shape[0] * HD
    mine_first = pl.multiple_of(idx_ref[0] * depth, depth)
    other_first = pl.multiple_of((1 - idx_ref[0]) * depth, depth)
    out_ref[...] = (
        jnp.dot(
            rows_of(mine_ref),
            w_ref[pl.ds(mine_first, depth), :],
            preferred_element_type=jnp.float32,
        )
        + jnp.dot(
            rows_of(other_ref),
            w_ref[pl.ds(other_first, depth), :],
            preferred_element_type=jnp.float32,
        )
    ).astype(out_ref.dtype)


def output_part(mine, other, w, row, col_block, width, dtype):
    heads, rows, _ = mine.shape
    bn = 512 if width % 512 == 0 else 256
    nb = width // bn
    idx = jnp.stack([jnp.int32(row), jnp.int32(col_block)])
    whole = pl.BlockSpec((heads, rows, HD), lambda j, i: (0, 0, 0))
    return pl.pallas_call(
        output_kernel,
        grid_spec=pltpu.PrefetchScalarGridSpec(
            num_scalar_prefetch=1,
            grid=(nb,),
            in_specs=[
                whole,
                whole,
                pl.BlockSpec((w.shape[0], bn), lambda j, i: (0, i[1] * nb + j)),
            ],
            out_specs=pl.BlockSpec((rows, bn), lambda j, i: (0, j)),
        ),
        out_shape=jax.ShapeDtypeStruct((rows, width), dtype),
        compiler_params=params(),
        cost_estimate=pl.CostEstimate(
            flops=2 * rows * w.shape[0] * width,
            bytes_accessed=width * (w.shape[0] * 2 + rows * 4),
            transcendentals=0,
        ),
    )(idx, mine, other, w)


def swap(x, axis):
    return lax.ppermute(x, axis, [(0, 1), (1, 0)])


def body(tokens, ln_gain, ln_bias, w_qkv, w_out):
    rows, quarter = tokens.shape
    row, col = lax.axis_index("row"), lax.axis_index("col")
    cols, seqs = lax.axis_size("col"), lax.axis_size("seq")
    model = quarter * cols * lax.axis_size("row")
    as_float = tokens.astype(jnp.float32)
    sums = lax.psum(
        jnp.stack([jnp.sum(as_float, axis=1), jnp.sum(as_float * as_float, axis=1)]),
        ("row", "col"),
    )
    token_mean = sums[0] / model
    spread = sums[1] / model - token_mean * token_mean
    normed = (
        (as_float - token_mean[:, None])
        * lax.rsqrt(spread + EPS)[:, None]
        * ln_gain.astype(jnp.float32)[None, :]
        + ln_bias.astype(jnp.float32)[None, :]
    ).astype(jnp.bfloat16)

    half = w_qkv.shape[2] // 2
    group_heads = half // HD
    by_head = group_heads % seqs == 0
    t_in = rows // IN_CHUNKS
    chunks = [normed[c * t_in : (c + 1) * t_in] for c in range(IN_CHUNKS)]
    if cols == 2:
        arrived = [swap(chunk, "col") for chunk in chunks]
        base = project(normed, w_qkv, None, 0, col, 0, 2 * half, jnp.float32, False)
        source = 1 - col
    else:
        arrived = [lax.all_gather(chunk, "col", axis=1, tiled=True) for chunk in chunks]
        base, source = None, 0

    owned = []
    for c in range(IN_CHUNKS):
        theirs = project(
            arrived[c], w_qkv, base, c, source, 1 - row, half, jnp.bfloat16, True
        )
        theirs = swap(theirs, "row")
        mine = project(arrived[c], w_qkv, base, c, source, row, half, jnp.float32, True)
        owned.append((mine + theirs.astype(jnp.float32)).astype(jnp.bfloat16))

    if by_head:
        split = [o.reshape(seqs, group_heads // seqs, 3, t_in, HD) for o in owned]
        split = [lax.all_to_all(o, "seq", 0, 0, tiled=True) for o in split]
        queries, kvs, k_at = split, split, 1
    else:
        queries = [o[None] for o in owned]
        kvs = [lax.all_gather(o[:, 1:], "seq", axis=0) for o in owned]
        k_at = 0

    finished = []
    for c in range(IN_CHUNKS):
        context = attend(queries[c], 0, kvs, k_at)
        if by_head:
            context = lax.all_to_all(context, "seq", 0, 0, tiled=True)
        context = context.reshape(group_heads, t_in, HD)
        other = swap(context, "row")
        residual = as_float[c * t_in : (c + 1) * t_in]
        if cols == 2:
            sent = output_part(context, other, w_out, row, 1 - col, quarter, jnp.bfloat16)
            sent = swap(sent, "col")
            kept = output_part(context, other, w_out, row, col, quarter, jnp.float32)
            summed = kept + sent.astype(jnp.float32)
        else:
            part = output_part(
                context, other, w_out, row, 0, w_out.shape[1], jnp.bfloat16
            )
            summed = lax.psum_scatter(
                part, "col", scatter_dimension=1, tiled=True
            ).astype(jnp.float32)
        finished.append((residual + summed).astype(jnp.bfloat16))
    return jnp.concatenate(finished, axis=0)


def solution(mesh):
    return jax.shard_map(
        body,
        mesh=mesh,
        in_specs=(
            P("seq", ("row", "col")),
            P(("row", "col")),
            P(("row", "col")),
            P(None, "row", "col"),
            P("col", "row"),
        ),
        out_specs=P("seq", ("row", "col")),
        check_vma=False,
    )
```

```python
import functools
import math

import jax
import jax.numpy as jnp
from jax import lax
from jax.experimental import pallas as pl
from jax.experimental.pallas import tpu as pltpu
from jax.sharding import PartitionSpec as P


HD = 128
EPS = 0.25
SIXTEENTHS = (7, 5, 4)
CHUNKS = len(SIXTEENTHS)
OUT_GROUPS = ((0,), (1,), (2,))
VMEM_LIMIT = 60 * 1024 * 1024


def params():
    return pltpu.CompilerParams(vmem_limit_bytes=VMEM_LIMIT)


def project_kernel(parts, idx_ref, *refs):
    x_refs, (w_ref, theirs_ref, mine_ref) = refs[:parts], refs[parts:]
    total = None
    for p, x_ref in enumerate(x_refs):
        depth = x_ref.shape[1]
        first = pl.multiple_of(idx_ref[p] * depth, depth)
        term = jnp.dot(
            x_ref[...], w_ref[0, pl.ds(first, depth), :], preferred_element_type=jnp.float32
        )
        total = term if total is None else total + term
    total = total.astype(jnp.bfloat16)

    def store(ref):
        for h in range(ref.shape[0]):
            ref[h, 0] = total[:, h * HD : (h + 1) * HD]

    pl.when(pl.program_id(0) == 0)(lambda: store(theirs_ref))
    pl.when(pl.program_id(0) == 1)(lambda: store(mine_ref))


def project(xs, row_blocks, w, row):
    rows = xs[0].shape[0]
    depth, width = w.shape[1], w.shape[2] // 2
    bn = min(1024, width)
    nb = width // bn
    parts = len(xs)
    idx = jnp.stack([jnp.int32(i) for i in (*row_blocks, 1 - row, row)])
    block = (bn // HD, 1, rows, HD)
    shape = jax.ShapeDtypeStruct((width // HD, 3, rows, HD), jnp.bfloat16)

    def theirs_at(s, k, j, i):
        return (jnp.where(s == 0, j, nb - 1), jnp.where(s == 0, k, 2), 0, 0)

    def mine_at(s, k, j, i):
        return (jnp.where(s == 0, 0, j), jnp.where(s == 0, 0, k), 0, 0)

    return pl.pallas_call(
        functools.partial(project_kernel, parts),
        grid_spec=pltpu.PrefetchScalarGridSpec(
            num_scalar_prefetch=1,
            grid=(2, 3, nb),
            in_specs=[pl.BlockSpec(x.shape, lambda s, k, j, i: (0, 0)) for x in xs]
            + [
                pl.BlockSpec(
                    (1, depth, bn), lambda s, k, j, i: (k, 0, i[parts + s] * nb + j)
                )
            ],
            out_specs=[pl.BlockSpec(block, theirs_at), pl.BlockSpec(block, mine_at)],
        ),
        out_shape=[shape, shape],
        compiler_params=params(),
        name="project",
        cost_estimate=pl.CostEstimate(
            flops=12 * rows * depth * width,
            bytes_accessed=12 * depth * width,
            transcendentals=0,
        ),
    )(idx, *xs, w)


def divisor(count, most):
    return next(n for n in range(max(1, min(count, most)), 0, -1) if count % n == 0)


def attend_kernel(parts, carried, final, q_ref, *refs):
    k_refs, v_refs, refs = refs[:parts], refs[parts : 2 * parts], refs[2 * parts :]
    bs, tq = q_ref.shape[0], q_ref.shape[3]
    scale = math.log2(math.e) / math.sqrt(HD)
    q = q_ref[:, 0, 0].reshape(bs * tq, HD)
    top = acc = None
    if carried:
        acc = refs[0][:, 0].reshape(bs * tq, 2 * HD)
        top = refs[1][:, 0].reshape(bs * tq, HD)[:, :1]
        refs = refs[2:]
    for k_ref, v_ref in zip(k_refs, v_refs):
        sources, tk = k_ref.shape[0], k_ref.shape[3]
        step = divisor(sources, 1024 // tk)
        for first in range(0, sources, step):
            keys = k_ref[first : first + step, 0, 0].reshape(step * tk, HD)
            values = v_ref[first : first + step, 0, 0].reshape(step * tk, HD)
            values = jnp.concatenate([values, jnp.ones_like(values)], axis=1)
            scores = lax.dot_general(
                q, keys, (((1,), (1,)), ((), ())), preferred_element_type=jnp.float32
            )
            block_top = jnp.max(scores, axis=1, keepdims=True) * scale
            new_top = block_top if top is None else jnp.maximum(top, block_top)
            weights = jnp.exp2(scores * scale - new_top).astype(jnp.bfloat16)
            part = jnp.dot(weights, values, preferred_element_type=jnp.float32)
            acc = part if top is None else acc * jnp.exp2(top - new_top) + part
            top = new_top
    if final:
        context = acc[:, :HD] / acc[:, HD:]
        refs[0][:, 0] = context.astype(jnp.bfloat16).reshape(bs, tq, HD)
    else:
        refs[0][:, 0] = acc.reshape(bs, tq, 2 * HD)
        refs[1][:, 0] = jnp.broadcast_to(top, (bs * tq, HD)).reshape(bs, tq, HD)


def attend(q, q_at, kvs, k_at, state=None, final=True):
    blocks, heads, _, tq, _ = q.shape
    bs = divisor(blocks, 1024 // tq)

    def kv_spec(kv, at):
        shape = (kv.shape[0], 1, 1, kv.shape[3], HD)
        return pl.BlockSpec(shape, lambda h, i: (0, h, at, 0, 0))

    def row_spec(width):
        return pl.BlockSpec((bs, 1, tq, width), lambda h, i: (i, h, 0, 0))

    def row_shape(width, dtype):
        return jax.ShapeDtypeStruct((blocks, heads, tq, width), dtype)

    state_specs = [row_spec(2 * HD), row_spec(HD)]
    key_count = sum(kv.shape[0] * kv.shape[3] for kv in kvs)
    pairs = heads * blocks * tq * key_count
    return pl.pallas_call(
        functools.partial(attend_kernel, len(kvs), state is not None, final),
        grid=(heads, blocks // bs),
        in_specs=[pl.BlockSpec((bs, 1, 1, tq, HD), lambda h, i: (i, h, q_at, 0, 0))]
        + [kv_spec(kv, k_at) for kv in kvs]
        + [kv_spec(kv, k_at + 1) for kv in kvs]
        + ([] if state is None else state_specs),
        out_specs=row_spec(HD) if final else state_specs,
        out_shape=row_shape(HD, jnp.bfloat16)
        if final
        else [row_shape(2 * HD, jnp.float32), row_shape(HD, jnp.float32)],
        name="attend",
        compiler_params=params(),
        cost_estimate=pl.CostEstimate(
            flops=8 * pairs * HD,
            bytes_accessed=4 * heads * key_count * HD + 4 * heads * blocks * tq * HD,
            transcendentals=pairs,
        ),
    )(q, *kvs, *kvs, *(() if state is None else state))


def output_kernel(idx_ref, mine_ref, other_ref, w_ref, out_ref):
    def rows_of(ref):
        return jnp.concatenate([ref[h] for h in range(ref.shape[0])], axis=1)

    depth = mine_ref.shape[0] * HD
    mine_first = pl.multiple_of(idx_ref[0] * depth, depth)
    other_first = pl.multiple_of((1 - idx_ref[0]) * depth, depth)
    out_ref[...] = (
        jnp.dot(
            rows_of(mine_ref),
            w_ref[pl.ds(mine_first, depth), :],
            preferred_element_type=jnp.float32,
        )
        + jnp.dot(
            rows_of(other_ref),
            w_ref[pl.ds(other_first, depth), :],
            preferred_element_type=jnp.float32,
        )
    ).astype(out_ref.dtype)


def output_part(mine, other, w, row, col_block, width, dtype):
    heads, rows, _ = mine.shape
    bn = next(n for n in (768, 512, 256) if width % n == 0)
    nb = width // bn
    idx = jnp.stack([jnp.int32(row), jnp.int32(col_block)])
    whole = pl.BlockSpec((heads, rows, HD), lambda j, i: (0, 0, 0))
    return pl.pallas_call(
        output_kernel,
        grid_spec=pltpu.PrefetchScalarGridSpec(
            num_scalar_prefetch=1,
            grid=(nb,),
            in_specs=[
                whole,
                whole,
                pl.BlockSpec((w.shape[0], bn), lambda j, i: (0, i[1] * nb + j)),
            ],
            out_specs=pl.BlockSpec((rows, bn), lambda j, i: (0, j)),
        ),
        out_shape=jax.ShapeDtypeStruct((rows, width), dtype),
        name="output_part",
        compiler_params=params(),
        cost_estimate=pl.CostEstimate(
            flops=2 * rows * w.shape[0] * width,
            bytes_accessed=width * (w.shape[0] * 2 + rows * 4),
            transcendentals=0,
        ),
    )(idx, mine, other, w)


def swap(x, axis):
    return lax.ppermute(x, axis, [(0, 1), (1, 0)])


def body(tokens, ln_gain, ln_bias, w_qkv, w_out):
    rows, quarter = tokens.shape
    row, col = lax.axis_index("row"), lax.axis_index("col")
    cols, seqs = lax.axis_size("col"), lax.axis_size("seq")
    model = quarter * cols * lax.axis_size("row")
    half = w_qkv.shape[2] // 2
    group_heads = half // HD
    by_head = group_heads % seqs == 0
    bounds = [rows * sum(SIXTEENTHS[:c]) // 16 for c in range(CHUNKS + 1)]
    pieces = [tokens[bounds[c] : bounds[c + 1]] for c in range(CHUNKS)]
    features = quarter
    scales = jnp.concatenate([ln_gain, ln_bias])
    if cols == 2:
        arrived = []
        for piece in pieces:
            arrived.append([piece, swap(piece, "col")])
        scales = [scales, swap(scales, "col")]
        blocks = [col, 1 - col]
    else:
        arrived = [[lax.all_gather(piece, "col", axis=1, tiled=True)] for piece in pieces]
        gathered = lax.all_gather(scales.reshape(2, quarter), "col", axis=1, tiled=True)
        features = quarter * cols
        scales = [gathered.reshape(2 * features)]
        blocks = [0]

    owned = []
    for held in arrived:
        floats = [x.astype(jnp.float32) for x in held]
        sums = jnp.stack(
            [
                sum(jnp.sum(x, axis=1) for x in floats),
                sum(jnp.sum(x * x, axis=1) for x in floats),
            ]
        )
        sums = (sums + swap(sums, "row")) / model
        inverse = lax.rsqrt(sums[1] - sums[0] * sums[0] + EPS)
        normed = [
            (
                (x - sums[0][:, None])
                * inverse[:, None]
                * scale[:features].astype(jnp.float32)[None, :]
                + scale[features:].astype(jnp.float32)[None, :]
            ).astype(jnp.bfloat16)
            for x, scale in zip(floats, scales)
        ]
        theirs, mine = project(normed, blocks, w_qkv, row)
        theirs = swap(theirs, "row")
        owned.append(
            (mine.astype(jnp.float32) + theirs.astype(jnp.float32)).astype(jnp.bfloat16)
        )

    if by_head:
        split = [o.reshape(seqs, group_heads // seqs, *o.shape[1:]) for o in owned]
        for c, o in enumerate(split):
            split[c] = lax.all_to_all(o, "seq", 0, 0, tiled=True)
        queries, kvs, k_at = split, split, 1
    else:
        queries = [o[None] for o in owned]
        kvs = [lax.all_gather(o[:, 1:], "seq", axis=0) for o in owned]
        k_at = 0

    states = []
    for c in range(CHUNKS - 1):
        states.append(attend(queries[c], 0, kvs[:-1], k_at, None, False))

    finished = []
    for group in OUT_GROUPS:
        contexts = []
        for c in group:
            if c < CHUNKS - 1:
                contexts.append(attend(queries[c], 0, kvs[-1:], k_at, states[c]))
            else:
                contexts.append(attend(queries[c], 0, kvs, k_at))
        context = jnp.concatenate(contexts, axis=2)
        first, last = bounds[group[0]], bounds[group[-1] + 1]
        if by_head:
            context = lax.all_to_all(context, "seq", 0, 0, tiled=True)
        context = context.reshape(group_heads, last - first, HD)
        other = swap(context, "row")
        if cols == 2:
            sent = output_part(
                context, other, w_out, row, 1 - col, quarter, jnp.bfloat16
            )
            sent = swap(sent, "col")
            kept = output_part(context, other, w_out, row, col, quarter, jnp.float32)
            summed = kept + sent.astype(jnp.float32)
        else:
            part = output_part(
                context, other, w_out, row, 0, w_out.shape[1], jnp.bfloat16
            )
            summed = lax.psum_scatter(
                part, "col", scatter_dimension=1, tiled=True
            ).astype(jnp.float32)
        residual = tokens[first:last].astype(jnp.float32)
        finished.append((residual + summed).astype(jnp.bfloat16))
    return jnp.concatenate(finished, axis=0)


def solution(mesh):
    return jax.shard_map(
        body,
        mesh=mesh,
        in_specs=(
            P("seq", ("row", "col")),
            P(("row", "col")),
            P(("row", "col")),
            P(None, "row", "col"),
            P("col", "row"),
        ),
        out_specs=P("seq", ("row", "col")),
        check_vma=False,
    )
```
